32 devices in a mesh: year: 16 (over z, y, x), space: 2 (over core).
Axes of the slice: x: 2, y: 2, z: 4, core: 2. Of those that a mesh axis runs over, the one named last changes fastest.
Arguments:
- thermal_reading: float32 [2048, 8192], P('year', 'space'), may hold values from -24 to 24
- yearday_position: int32 [2048], P('year'), may hold values from 0 to 29, as said below
- usable_observation_tally: int32 [2048], P('year'), may hold values from 1 to 24
- location_surface_factor: float32 [8192], P('space'), may hold values from 0.2 to 5.4
Outputs:
- normalized_departure: float32 [2048, 8192], P('year', 'space')
- spread: float32 [2048], P('year')
The draws below stay inside these ranges and needn't reach their ends.
Inputs may be any that keep to these rules, and one draw needn't show every extreme that they name: `yearday_position`: every day of 0 to 29 is the day of at least one step.
All inputs are finite; a program needn't handle non-finite values.
Results may differ from the reference program's by a relative error of at most 0.0003.
Values sent between devices are 32-bit elements; how exact they have to be, the bound alone decides.
A program may use at most 64 MiB of HBM per device.

```python
import jax
import jax.numpy as jnp
from jax import lax

DAYS = 30
NUM_DATES = 2048
NUM_LOCATIONS = 8192


def draw_yearday_position(key, part):
    first = jax.random.fold_in(key, 11)
    second = jax.random.fold_in(key, 12)
    days_drawn = jax.random.randint(first, (NUM_DATES,), 0, DAYS).astype(jnp.int32)
    places = jax.random.permutation(second, NUM_DATES)[:DAYS]
    return days_drawn.at[places].set(jnp.arange(DAYS, dtype=jnp.int32))


def draw_location_surface_factor(key, part):
    position = jnp.arange(NUM_LOCATIONS, dtype=jnp.float32)
    rising = 1.0 + 2.0 * position / max(NUM_LOCATIONS - 1, 1)
    jitter = jax.random.uniform(jax.random.fold_in(key, 22), (NUM_LOCATIONS,), jnp.float32, 0.6, 1.4)
    return (rising * jitter).astype(jnp.float32)


def set_ends(result, own_key, smallest, high):
    place = [jax.random.randint(jax.random.fold_in(own_key, axis), (), 0, length) for axis, length in enumerate(result.shape)]
    longest = result.shape.index(max(result.shape))
    next_to = place[:longest] + [(place[longest] + 1) % result.shape[longest]] + place[longest + 1:]
    return result.at[tuple(place)].set(smallest).at[tuple(next_to)].set(high)


def shard_levels(key, shape, shards, low, high):
    def one(dim, shards_of):
        draws = jax.random.uniform(jax.random.fold_in(jax.random.fold_in(key, 6), dim), (shards_of,), jnp.float32, low / len(shards), high / len(shards))
        return jnp.repeat(jnp.exp(draws), shape[dim] // shards_of).reshape((-1,) + (1,) * (len(shape) - dim - 1))

    gain = one(*shards[0])
    for cut in shards[1:]:
        gain = gain * one(*cut)
    return gain


def normal_values(key, extent, scale, limit, cuts=(), kind=jnp.bfloat16):
    values = jax.random.normal(key, extent, jnp.float32) * scale
    if len(cuts) > 0:
        values = shard_levels(key, extent, cuts, -0.22, 0.18) * values
    return jnp.clip(values, min=-limit, max=limit).astype(kind)


def setup_inputs(seed: int = 0) -> dict:
    key_of = jax.random.split(jax.random.key(seed), 5)
    return {
        "thermal_reading": normal_values(key_of[0], (NUM_DATES, NUM_LOCATIONS), 4.0, 24.0, ((0, 16), (1, 2)), jnp.float32),
        "yearday_position": draw_yearday_position(jax.random.fold_in(key_of[4], 71), 0),
        "usable_observation_tally": set_ends(jax.random.randint(key_of[2], (NUM_DATES,), 1, 25), jax.random.fold_in(key_of[2], 1), 1, 24).astype(jnp.int32),
        "location_surface_factor": draw_location_surface_factor(jax.random.fold_in(key_of[4], 71), 0),
    }


def reference(thermal_reading, yearday_position, usable_observation_tally, location_surface_factor):
    days_row = jnp.arange(DAYS, dtype=jnp.int32)
    yearday_onehot = (yearday_position[None, :] == days_row[:, None]).astype(jnp.float32)
    observation_tally = usable_observation_tally.astype(jnp.float32)
    surface_scaled_product = jnp.dot(yearday_onehot * observation_tally[None, :], thermal_reading, precision=lax.Precision.HIGHEST)
    hour_total = jnp.sum(yearday_onehot * observation_tally[None, :], axis=1)

    def extremes(which_day):
        picked_elements = (yearday_position == which_day)[:, None]
        ceiling_bound = jnp.max(jnp.where(picked_elements, thermal_reading, -jnp.inf), axis=0)
        bottom_bound = jnp.min(jnp.where(picked_elements, thermal_reading, jnp.inf), axis=0)
        return ceiling_bound, bottom_bound

    yearday_ceiling, yearday_floor = lax.map(extremes, days_row)
    day_mean = surface_scaled_product / hour_total[:, None]
    day_scale = 4.0 / (yearday_ceiling - yearday_floor + 1.0)
    dated_average = jnp.take(day_mean, yearday_position, axis=0)
    dated_deviation = jnp.take(day_scale, yearday_position, axis=0)
    normalized_departure = (thermal_reading - dated_average) * dated_deviation
    spread = jnp.sum(location_surface_factor[None, :] * normalized_departure * normalized_departure, axis=1) / jnp.sum(location_surface_factor)
    return normalized_departure, spread
```

```python
import functools

import jax
import jax.numpy as jnp
from jax import lax
from jax.experimental import pallas as pl
from jax.experimental.pallas import tpu as pltpu
from jax.sharding import PartitionSpec as P

DAYS = 30
LANES = 128
DAY_PARTS = 2
DAY_SLOTS = 32
PART_DAYS = DAYS // DAY_PARTS
HOURS_ROW = PART_DAYS
HIGH_ROW = -(-(PART_DAYS + 1) // 8) * 8
LOW_ROW = 2 * HIGH_ROW
STAT_ROWS = 3 * HIGH_ROW
TABLE_ROWS = 2 * HIGH_ROW
LAG = 3


def pitch_of(rows):
    return rows if rows // 8 % 2 else rows + 8


STAT_PITCH = pitch_of(DAY_PARTS * STAT_ROWS)
TABLE_PITCH = pitch_of(DAY_PARTS * TABLE_ROWS)
MESH = pl.DeviceIdType.MESH

BLOCKS = 8


def stats_kernel(chunks, code_hbm, x_hbm, out_ref, acc, x_ref, code_ref, sems):
    steps = code_ref.shape[0]
    block = steps // BLOCKS
    copies = [pltpu.make_async_copy(code_hbm, code_ref, sems.at[BLOCKS])]
    loads = []
    for g in range(BLOCKS):
        rows = pl.ds(g * block * chunks, block * chunks)
        loads.append(pltpu.make_async_copy(x_hbm.at[rows], x_ref.at[rows], sems.at[g]))
    for copy in copies + loads:
        copy.start()
    acc[0:DAYS] = jnp.zeros((DAYS, chunks, LANES), jnp.float32)
    acc[DAYS:] = jnp.full((2 * DAYS, chunks, LANES), -jnp.inf, jnp.float32)
    lane = lax.broadcasted_iota(jnp.int32, (8, LANES), 1)

    def step(s, hours):
        code = code_ref[s]
        d = code & (DAY_SLOTS - 1)
        tally = (code // DAY_SLOTS).astype(jnp.float32)
        row = x_ref[pl.ds((s // 8) * (8 * chunks) + s % 8, chunks, stride=8), :]
        acc[d] = acc[d] + tally * row
        acc[DAYS + d] = jnp.maximum(acc[DAYS + d], row)
        acc[2 * DAYS + d] = jnp.maximum(acc[2 * DAYS + d], -row)
        return hours + jnp.where(lane == d, tally, 0.0)

    for copy in copies:
        copy.wait()
    hours = jnp.zeros((8, LANES), jnp.float32)
    for g in range(BLOCKS):
        loads[g].wait()
        hours = lax.fori_loop(g * block, (g + 1) * block, step, hours)
    hours = jnp.broadcast_to(hours[0:1], (chunks, LANES))
    for q in range(DAY_PARTS):

        def put(row, value):
            out_ref[pl.ds(q * STAT_ROWS + row, chunks, stride=STAT_PITCH), :] = value

        for k, first in enumerate((0, HIGH_ROW, LOW_ROW)):
            for j in range(PART_DAYS):
                put(first + j, acc[k * DAYS + q * PART_DAYS + j])
        for first in (0, HIGH_ROW, LOW_ROW):
            for row in range(first + PART_DAYS, first + HIGH_ROW):
                put(row, hours)


def flipped(me, mask):
    target = me
    for i in range(mask.bit_length()):
        if mask >> i & 1:
            target = target + (1 - 2 * ((me // (1 << i)) % 2)) * (1 << i)
    return target


def subsets_of(dims):
    masks = [0]
    for i in dims:
        masks += [m | (1 << i) for m in masks]
    return masks


def plan_of(groups, chunks):
    bits = groups.bit_length() - 1
    assert 1 << bits == groups and bits >= 2
    pieces = groups // 2
    assert chunks % pieces == 0
    parts = []
    for t in range(chunks // pieces):
        for q in range(DAY_PARTS):
            first = len(parts) % (bits - 1)
            subs = subsets_of([i for i in range(bits - 1) if i != first])
            parts.append((t, q, 1 << first, subs))
    return pieces, groups // 2, parts


def exchange_kernel(
    groups, chunks, stats_ref, table_ref, work, recv, s1, r1, s2, r2, s3, r3, s4, r4, s5, r5
):
    me = lax.axis_index("year")
    pieces, across, parts = plan_of(groups, chunks)
    low = me % pieces
    slots = len(parts[0][3])

    peers = {across}
    for _, _, first, subs in parts:
        peers |= {first} | set(subs[1:])
    peers = sorted(peers)
    barrier = pltpu.get_barrier_semaphore()
    for mask in peers:
        pl.semaphore_signal(
            barrier, inc=1, device_id={"year": flipped(me, mask)}, device_id_type=MESH
        )
    pl.semaphore_wait(barrier, len(peers))

    copies = []

    def send(mask, source, target, send_sem, recv_sem):
        copy = pltpu.make_async_remote_copy(
            src_ref=source,
            dst_ref=target,
            send_sem=send_sem,
            recv_sem=recv_sem,
            device_id={"year": flipped(me, mask)},
            device_id_type=MESH,
        )
        copy.start()
        copies.append(copy)
        return copy

    sums = slice(0, HIGH_ROW)
    tops = slice(HIGH_ROW, STAT_ROWS)

    def stat_at(p, mask):
        t, q, _, _ = parts[p]
        return t * pieces + flipped(low, mask), q * STAT_ROWS

    halved, grouped, crossed, shared, doubled = {}, {}, {}, {}, {}

    def halve_send(p):
        _, _, first, subs = parts[p]
        for k in list(range(1, slots)) + [0]:
            at, row = stat_at(p, first | subs[k])
            halved[p, k] = send(
                first,
                stats_ref.at[at, pl.ds(row, STAT_ROWS)],
                recv.at[p, k],
                s1.at[p, k],
                r1.at[p, k],
            )

    def group_send(p):
        _, _, first, subs = parts[p]
        for k in list(range(1, slots)) + [0]:
            at, row = stat_at(p, subs[k])
            halved[p, k].wait_recv()
            work[p, k, sums] = stats_ref[at, row : row + HIGH_ROW] + recv[p, k, sums]
            work[p, k, tops] = jnp.maximum(
                stats_ref[at, row + HIGH_ROW : row + STAT_ROWS], recv[p, k, tops]
            )
            if k:
                grouped[p, k] = send(
                    subs[k], work.at[p, k], recv.at[p, slots + k], s2.at[p, k], r2.at[p, k]
                )

    def cross_send(p):
        add, top = work[p, 0, sums], work[p, 0, tops]
        for k in range(1, slots):
            grouped[p, k].wait_recv()
            add = add + recv[p, slots + k, sums]
            top = jnp.maximum(top, recv[p, slots + k, tops])
        work[p, slots, sums] = add
        work[p, slots, tops] = top
        crossed[p] = send(across, work.at[p, slots], recv.at[p, slots], s3.at[p], r3.at[p])

    def table_at(p, mask):
        t, q, _, _ = parts[p]
        return table_ref.at[
            t * pieces + flipped(low, mask), pl.ds(q * TABLE_ROWS, TABLE_ROWS)
        ]

    eye = lax.broadcasted_iota(jnp.int32, (HIGH_ROW, LANES), 0)
    lane = lax.broadcasted_iota(jnp.int32, (HIGH_ROW, LANES), 1)

    def share_send(p):
        t, q, first, subs = parts[p]
        crossed[p].wait_recv()
        add = work[p, slots, sums] + recv[p, slots, sums]
        top = jnp.maximum(work[p, slots, tops], recv[p, slots, tops])
        hours = jnp.sum(
            jnp.where(lane == eye + q * PART_DAYS, add[HOURS_ROW : HOURS_ROW + 1], 0.0),
            axis=1,
            keepdims=True,
        )
        mean = add / hours
        scale = 4.0 / (top[0:HIGH_ROW] + top[HIGH_ROW:] + 1.0)
        at, row = t * pieces + low, q * TABLE_ROWS
        table_ref[at, row : row + HIGH_ROW] = mean
        table_ref[at, row + HIGH_ROW : row + TABLE_ROWS] = scale
        for k in range(1, slots):
            shared[p, k] = send(subs[k], table_at(p, 0), table_at(p, 0), s4.at[p, k], r4.at[p, k])
        doubled[p, 0] = send(first, table_at(p, 0), table_at(p, 0), s5.at[p, 0], r5.at[p, 0])

    def double_send(p):
        _, _, first, subs = parts[p]
        for k in range(1, slots):
            shared[p, k].wait_recv()
            where = table_at(p, subs[k])
            doubled[p, k] = send(first, where, where, s5.at[p, k], r5.at[p, k])

    def finish(p):
        for k in range(slots):
            doubled[p, k].wait_recv()

    for p in range(len(parts)):
        halve_send(p)
    stages = [group_send, cross_send, share_send, double_send, finish]
    for at in range(len(parts) + LAG * (len(stages) - 1)):
        for i in reversed(range(len(stages))):
            p = at - LAG * i
            if 0 <= p < len(parts):
                stages[i](p)
    for copy in copies:
        copy.wait_send()


def apply_kernel(chunks, pos_ref, x_ref, table_ref, weight_ref, out_hbm, spread_ref, out_ref, sems):
    steps = pos_ref.shape[0]
    weight = weight_ref[...]
    block = steps // BLOCKS

    def step(s, carry):
        d = pos_ref[s]
        q = d // PART_DAYS
        row = q * TABLE_ROWS + (d - q * PART_DAYS)
        at = pl.ds((s // 8) * (8 * chunks) + s % 8, chunks, stride=8)
        mean = table_ref[pl.ds(row, chunks, stride=TABLE_PITCH), :]
        scale = table_ref[pl.ds(row + HIGH_ROW, chunks, stride=TABLE_PITCH), :]
        departure = (x_ref[at, :] - mean) * scale
        out_ref[at, :] = departure
        squares = weight * departure * departure
        spread_ref[pl.ds(s, 1), :] = jnp.sum(squares, axis=0, keepdims=True)
        return carry

    stores = []
    for g in range(BLOCKS):
        lax.fori_loop(g * block, (g + 1) * block, step, 0, unroll=4)
        rows = pl.ds(g * block * chunks, block * chunks)
        store = pltpu.make_async_copy(out_ref.at[rows], out_hbm.at[rows], sems.at[g])
        store.start()
        stores.append(store)
    for store in stores:
        store.wait()


def spread_kernel(peers, partial_ref, weight_ref, out_ref, mine, theirs, send, recv):
    me = lax.axis_index("space")
    others = [(me + k) % peers for k in range(1, peers)]
    barrier = pltpu.get_barrier_semaphore()
    for p in others:
        pl.semaphore_signal(barrier, inc=1, device_id={"space": p}, device_id_type=MESH)
    steps = partial_ref.shape[0]
    area = jnp.sum(weight_ref[...], axis=0, keepdims=True)
    area = jnp.broadcast_to(jnp.sum(area, axis=1, keepdims=True), (8, steps))
    sums = jnp.broadcast_to(jnp.sum(partial_ref[...].T, axis=0, keepdims=True), (8, steps))
    row = lax.broadcasted_iota(jnp.int32, (8, steps), 0)
    both = jnp.where(row == 0, sums, area)
    mine[...] = both
    if others:
        pl.semaphore_wait(barrier, len(others))
    copies = []
    for k, p in enumerate(others):
        copy = pltpu.make_async_remote_copy(
            src_ref=mine,
            dst_ref=theirs.at[k],
            send_sem=send.at[k],
            recv_sem=recv.at[k],
            device_id={"space": p},
            device_id_type=MESH,
        )
        copy.start()
        copies.append(copy)
    for k, copy in enumerate(copies):
        copy.wait()
        both = both + theirs[k]
    out_ref[...] = both[0:1] / both[1:2]


def on_device(thermal_reading, yearday_position, usable_observation_tally, location_surface_factor):
    groups = lax.axis_size("year")
    steps, cells = thermal_reading.shape
    chunks = cells // LANES
    assert steps % (8 * BLOCKS) == 0 and chunks * LANES == cells
    _, _, parts = plan_of(groups, chunks)
    n_parts, slots = len(parts), len(parts[0][3])

    tiles = thermal_reading.reshape(steps // 8, 8, chunks, LANES).transpose(0, 2, 1, 3)
    tiles = tiles.reshape(steps * chunks, LANES)
    vmem = pl.BlockSpec(memory_space=pltpu.VMEM)
    smem = pl.BlockSpec(memory_space=pltpu.SMEM)

    hbm = pl.BlockSpec(memory_space=pltpu.HBM)
    stats = pl.pallas_call(
        functools.partial(stats_kernel, chunks),
        out_shape=jax.ShapeDtypeStruct((chunks * STAT_PITCH, LANES), jnp.float32),
        in_specs=[hbm, hbm],
        out_specs=vmem,
        scratch_shapes=[
            pltpu.VMEM((3 * DAYS, chunks, LANES), jnp.float32),
            pltpu.VMEM((steps * chunks, LANES), jnp.float32),
            pltpu.SMEM((steps,), jnp.int32),
            pltpu.SemaphoreType.DMA((BLOCKS + 1,)),
        ],
        compiler_params=pltpu.CompilerParams(vmem_limit_bytes=16 << 20),
        name="day_stats",
    )(yearday_position + DAY_SLOTS * usable_observation_tally, tiles)

    weight = location_surface_factor.reshape(chunks, LANES)
    table = pl.pallas_call(
        functools.partial(exchange_kernel, groups, chunks),
        out_shape=jax.ShapeDtypeStruct((chunks, TABLE_PITCH, LANES), jnp.float32),
        in_specs=[vmem],
        out_specs=vmem,
        scratch_shapes=[
            pltpu.VMEM((n_parts, slots + 1, STAT_ROWS, LANES), jnp.float32),
            pltpu.VMEM((n_parts, 2 * slots, STAT_ROWS, LANES), jnp.float32),
            pltpu.SemaphoreType.DMA((n_parts, slots)),
            pltpu.SemaphoreType.DMA((n_parts, slots)),
            pltpu.SemaphoreType.DMA((n_parts, slots)),
            pltpu.SemaphoreType.DMA((n_parts, slots)),
            pltpu.SemaphoreType.DMA((n_parts,)),
            pltpu.SemaphoreType.DMA((n_parts,)),
            pltpu.SemaphoreType.DMA((n_parts, slots)),
            pltpu.SemaphoreType.DMA((n_parts, slots)),
            pltpu.SemaphoreType.DMA((n_parts, slots)),
            pltpu.SemaphoreType.DMA((n_parts, slots)),
        ],
        compiler_params=pltpu.CompilerParams(
            collective_id=0, has_side_effects=True, vmem_limit_bytes=16 << 20
        ),
        name="day_exchange",
    )(stats.reshape(chunks, STAT_PITCH, LANES))

    departure, partial = pl.pallas_call(
        functools.partial(apply_kernel, chunks),
        out_shape=(
            jax.ShapeDtypeStruct((steps * chunks, LANES), jnp.float32),
            jax.ShapeDtypeStruct((steps, LANES), jnp.float32),
        ),
        in_specs=[smem, vmem, vmem, vmem],
        out_specs=(hbm, vmem),
        scratch_shapes=[
            pltpu.VMEM((steps * chunks, LANES), jnp.float32),
            pltpu.SemaphoreType.DMA((BLOCKS,)),
        ],
        compiler_params=pltpu.CompilerParams(vmem_limit_bytes=16 << 20),
        name="day_apply",
    )(
        yearday_position,
        tiles,
        table.reshape(chunks * TABLE_PITCH, LANES),
        weight,
    )
    normalized_departure = (
        departure.reshape(steps // 8, chunks, 8, LANES).transpose(0, 2, 1, 3).reshape(steps, cells)
    )
    peers = lax.axis_size("space")
    others = max(peers - 1, 1)
    spread = pl.pallas_call(
        functools.partial(spread_kernel, peers),
        out_shape=jax.ShapeDtypeStruct((1, steps), jnp.float32),
        in_specs=[vmem, vmem],
        out_specs=vmem,
        scratch_shapes=[
            pltpu.VMEM((8, steps), jnp.float32),
            pltpu.VMEM((others, 8, steps), jnp.float32),
            pltpu.SemaphoreType.DMA((others,)),
            pltpu.SemaphoreType.DMA((others,)),
        ],
        compiler_params=pltpu.CompilerParams(
            collective_id=1, has_side_effects=True, vmem_limit_bytes=16 << 20
        ),
        name="area_spread",
    )(partial, weight)
    return normalized_departure, spread.reshape(steps)


def solution(mesh):
    return jax.shard_map(
        on_device,
        mesh=mesh,
        in_specs=(P("year", "space"), P("year"), P("year"), P("space")),
        out_specs=(P("year", "space"), P("year")),
        check_vma=False,
    )
```

```python
import functools

import jax
import jax.numpy as jnp
from jax import lax
from jax.experimental import pallas as pl
from jax.experimental.pallas import tpu as pltpu
from jax.sharding import PartitionSpec as P

DAYS = 30
LANES = 128
DAY_PARTS = 2
PART_DAYS = DAYS // DAY_PARTS
HOURS_ROW = PART_DAYS
HIGH_ROW = -(-(PART_DAYS + 1) // 8) * 8
LOW_ROW = 2 * HIGH_ROW
STAT_ROWS = 3 * HIGH_ROW
TABLE_ROWS = 2 * HIGH_ROW
FAR = 3e38
MESH = pl.DeviceIdType.MESH


def pitch_of(rows):
    return rows if rows // 8 % 2 else rows + 8


STAT_PITCH = pitch_of(DAY_PARTS * STAT_ROWS)
TABLE_PITCH = pitch_of(DAY_PARTS * TABLE_ROWS)


def flipped(me, mask):
    target = me
    for i in range(mask.bit_length()):
        if mask >> i & 1:
            target = target + (1 - 2 * ((me // (1 << i)) % 2)) * (1 << i)
    return target


def subsets_of(dims):
    masks = [0]
    for i in dims:
        masks += [m | (1 << i) for m in masks]
    return masks


def plan_of(groups, chunks):
    bits = groups.bit_length() - 1
    assert 1 << bits == groups and bits >= 2
    pieces = groups // 2
    assert chunks % pieces == 0
    parts = []
    for t in range(chunks // pieces):
        for q in range(DAY_PARTS):
            first = len(parts) % (bits - 1)
            subs = subsets_of([i for i in range(bits - 1) if i != first])
            parts.append((t, q, 1 << first, subs))
    return pieces, groups // 2, parts


def sort_steps(pieces, pos, tally, order, factors):
    n = pos.shape[-1]
    lane = lax.broadcasted_iota(jnp.int32, (n, n), 1)
    step = lax.broadcasted_iota(jnp.int32, (n, n), 0)
    wide = jnp.broadcast_to(pos, (n, n))
    day = wide.T
    hours = jnp.broadcast_to(tally, (n, n)).T

    def total(values):
        return jnp.sum(values, axis=0, keepdims=True)

    rank = total(jnp.where(day * n + step < wide * n + lane, 1, 0))
    here = jnp.broadcast_to(rank, (n, n)).T == lane
    place = total(jnp.where(here, step // 8 * (8 * pieces) + step % 8, 0))
    sorted_day = total(jnp.where(here, day, 0))
    sorted_tally = total(jnp.where(here, hours, 0))
    of_day = day == lane
    count = total(jnp.where(of_day, 1, 0))
    last = jnp.where(count > 0, total(jnp.where(day <= lane, 1, 0)) - 1, n)
    row = pos
    for q in range(1, DAY_PARTS):
        row = row + jnp.where(pos >= q * PART_DAYS, TABLE_ROWS - PART_DAYS, 0)
    before = pltpu.roll(jnp.broadcast_to(sorted_day, (8, n)), 1, 1)[0:1]
    kept = jnp.where((before == sorted_day) & (lane[0:1] > 0), 1.0, 0.0)
    order[0:1] = place
    order[1:2] = last
    order[2:3] = row
    factors[0:1] = sorted_tally.astype(jnp.float32)
    factors[1:2] = kept
    factors[2:3] = (kept - 1.0) * FAR
    return total(jnp.where(of_day, hours, 0)).astype(jnp.float32)


def climate_kernel(
    groups,
    spaces,
    chunks,
    x_hbm,
    pos_hbm,
    tally_hbm,
    weight_hbm,
    out_ref,
    spread_ref,
    *scratch,
):
    pieces, across, parts = plan_of(groups, chunks)
    tiles = chunks // pieces
    xs, tables = scratch[:tiles], scratch[tiles : 2 * tiles]
    (
        pos_ref, tally_ref, weight_ref, order_ref, factor_ref, order, factors,
        runs, stats, work, recv, squares, sums, mine, theirs,
        xsem, insem, sent, r1, r2, r3, r4, r5, ss, rs,
    ) = scratch[2 * tiles :]
    steps = pos_ref.shape[-1]
    me = lax.axis_index("year")
    cell_group = lax.axis_index("space")
    low = me % pieces
    slots = len(parts[0][3])

    small = [
        pltpu.make_async_copy(pos_hbm, pos_ref, insem.at[0]),
        pltpu.make_async_copy(tally_hbm, tally_ref, insem.at[1]),
        pltpu.make_async_copy(weight_hbm, weight_ref, insem.at[2]),
    ]
    small[0].start()
    small[1].start()
    loads = []
    for t in range(tiles):
        rows = pl.ds(t * pieces * 8, pieces * 8)
        loads.append(pltpu.make_async_copy(x_hbm.at[:, rows], xs[t], xsem.at[t]))
        loads[t].start()
    small[2].start()

    peers = {across}
    for _, _, first, subs in parts:
        peers |= {first} | set(subs[1:])
    others = [(cell_group + k) % spaces for k in range(1, spaces)]
    barrier = pltpu.get_barrier_semaphore()
    for mask in sorted(peers):
        pl.semaphore_signal(
            barrier, inc=1, device_id={"year": flipped(me, mask)}, device_id_type=MESH
        )
    for p in others:
        pl.semaphore_signal(barrier, inc=1, device_id={"space": p}, device_id_type=MESH)

    small[0].wait()
    small[1].wait()
    hours = sort_steps(pieces, pos_ref[...], tally_ref[...], order_ref, factor_ref)
    to_scalar = [
        pltpu.make_async_copy(order_ref, order, insem.at[3]),
        pltpu.make_async_copy(factor_ref, factors, insem.at[4]),
    ]
    for copy in to_scalar:
        copy.start()
    hours = jnp.broadcast_to(hours, (pieces, LANES))
    runs[0, steps] = jnp.zeros((pieces, LANES), jnp.float32)
    runs[1, steps] = jnp.full((pieces, LANES), -jnp.inf, jnp.float32)
    runs[2, steps] = jnp.full((pieces, LANES), jnp.inf, jnp.float32)
    for copy in to_scalar:
        copy.wait()

    def tile_stats(t):
        loads[t].wait()
        readings = xs[t].reshape(steps * pieces, LANES)

        def scan(r, carry):
            add, top, bottom = carry
            row = readings[pl.ds(order[0, r], pieces, stride=8), :]
            far = factors[2, r]
            add = add * factors[1, r] + factors[0, r] * row
            top = jnp.maximum(row, top + far)
            bottom = jnp.minimum(row, bottom - far)
            runs[0, r] = add
            runs[1, r] = top
            runs[2, r] = bottom
            return add, top, bottom

        zero = jnp.zeros((pieces, LANES), jnp.float32)
        lax.fori_loop(0, steps, scan, (zero, zero, zero), unroll=8)

        def put(row, value):
            stats[pl.ds(t * pieces * STAT_PITCH + row, pieces, stride=STAT_PITCH), :] = value

        for d in range(DAYS):
            at = order[1, d]
            row = d // PART_DAYS * STAT_ROWS + d % PART_DAYS
            put(row, runs[0, at])
            put(row + HIGH_ROW, runs[1, at])
            put(row + LOW_ROW, -runs[2, at])
        for q in range(DAY_PARTS):
            for first in (0, HIGH_ROW, LOW_ROW):
                for row in range(first + PART_DAYS, first + HIGH_ROW):
                    put(q * STAT_ROWS + row, hours)

    def landed(like, sem):
        pltpu.make_async_copy(like, like, sem).wait()

    def send(mask, source, target, send_sem, recv_sem):
        copy = pltpu.make_async_remote_copy(
            src_ref=source,
            dst_ref=target,
            send_sem=send_sem,
            recv_sem=recv_sem,
            device_id={"year": flipped(me, mask)},
            device_id_type=MESH,
        )
        copy.start()

    def stat_row(p, mask):
        t, q, _, _ = parts[p]
        return pl.multiple_of((t * pieces + flipped(low, mask)) * STAT_PITCH + q * STAT_ROWS, 8)

    def halve_send(p):
        _, _, first, subs = parts[p]
        for k in list(range(1, slots)) + [0]:
            send(
                first,
                stats.at[pl.ds(stat_row(p, first | subs[k]), STAT_ROWS)],
                recv.at[p, k],
                sent.at[0],
                r1.at[p],
            )

    add_rows = slice(0, HIGH_ROW)
    top_rows = slice(HIGH_ROW, STAT_ROWS)

    def group_send(p):
        _, _, _, subs = parts[p]
        landed(recv.at[p, pl.ds(0, slots)], r1.at[p])
        for k in list(range(1, slots)) + [0]:
            row = stat_row(p, subs[k])
            work[p, k, add_rows] = stats[pl.ds(row, HIGH_ROW)] + recv[p, k, add_rows]
            work[p, k, top_rows] = jnp.maximum(
                stats[pl.ds(row + HIGH_ROW, 2 * HIGH_ROW)], recv[p, k, top_rows]
            )
            if k:
                send(subs[k], work.at[p, k], recv.at[p, slots + k], sent.at[1], r2.at[p])

    def cross_send(p):
        add, top = work[p, 0, add_rows], work[p, 0, top_rows]
        landed(recv.at[p, pl.ds(slots + 1, slots - 1)], r2.at[p])
        for k in range(1, slots):
            add = add + recv[p, slots + k, add_rows]
            top = jnp.maximum(top, recv[p, slots + k, top_rows])
        work[p, slots, add_rows] = add
        work[p, slots, top_rows] = top
        send(across, work.at[p, slots], recv.at[p, slots], sent.at[2], r3.at[p])

    def table_at(p, mask):
        t, q, _, _ = parts[p]
        row = pl.multiple_of(flipped(low, mask) * TABLE_PITCH + q * TABLE_ROWS, 8)
        return tables[t].at[pl.ds(row, TABLE_ROWS)]

    eye = lax.broadcasted_iota(jnp.int32, (HIGH_ROW, LANES), 0)
    lane = lax.broadcasted_iota(jnp.int32, (HIGH_ROW, LANES), 1)

    def share_send(p):
        _, q, first, subs = parts[p]
        landed(recv.at[p, slots], r3.at[p])
        add = work[p, slots, add_rows] + recv[p, slots, add_rows]
        top = jnp.maximum(work[p, slots, top_rows], recv[p, slots, top_rows])
        day_hours = jnp.sum(
            jnp.where(lane == eye + q * PART_DAYS, add[HOURS_ROW : HOURS_ROW + 1], 0.0),
            axis=1,
            keepdims=True,
        )
        mean = add / day_hours
        scale = 4.0 / (top[0:HIGH_ROW] + top[HIGH_ROW:] + 1.0)
        own = table_at(p, 0)
        own[0:HIGH_ROW] = mean
        own[HIGH_ROW:TABLE_ROWS] = scale
        for k in range(1, slots):
            send(subs[k], own, own, sent.at[3], r4.at[p])
        send(first, own, own, sent.at[4], r5.at[p])

    def double_send(p):
        t, _, first, subs = parts[p]
        landed(tables[t].at[pl.ds(0, (slots - 1) * TABLE_ROWS)], r4.at[p])
        for k in range(1, slots):
            where = table_at(p, subs[k])
            send(first, where, where, sent.at[4], r5.at[p])

    def finish(p):
        landed(tables[parts[p][0]].at[pl.ds(0, slots * TABLE_ROWS)], r5.at[p])

    def tile_apply(t):
        weight = weight_ref[t * pieces : (t + 1) * pieces, :]
        readings = xs[t].reshape(steps * pieces, LANES)

        def group(g, carry):
            for i in range(8):
                s = g * 8 + i
                row = order[2, s]
                mean = tables[t][pl.ds(row, pieces, stride=TABLE_PITCH), :]
                scale = tables[t][pl.ds(row + HIGH_ROW, pieces, stride=TABLE_PITCH), :]
                reading = readings[pl.ds(g * (pieces * 8) + i, pieces, stride=8), :]
                departure = (reading - mean) * scale
                at = g * (chunks * 8) + (t * pieces * 8 + i)
                out_ref[pl.ds(at, pieces, stride=8), :] = departure
                square = weight * departure * departure
                if t:
                    square = square + squares[s]
                squares[s] = square
            return carry

        lax.fori_loop(0, steps // 8, group, 0)

    pl.semaphore_wait(barrier, len(peers) + len(others))
    for t in range(tiles):
        tile_stats(t)
        for p in range(len(parts)):
            if parts[p][0] == t:
                halve_send(p)
    for stage in (group_send, cross_send, share_send, double_send):
        for p in range(len(parts)):
            stage(p)
    small[2].wait()
    for t in range(tiles):
        for p in range(len(parts)):
            if parts[p][0] == t:
                finish(p)
        tile_apply(t)

    for g in range(steps // 8):
        sums[g * 8 : g * 8 + 8] = jnp.sum(squares[g * 8 : g * 8 + 8], axis=1)
    area = jnp.sum(weight_ref[...], axis=0, keepdims=True)
    area = jnp.broadcast_to(jnp.sum(area, axis=1, keepdims=True), (8, steps))
    total = jnp.broadcast_to(jnp.sum(sums[...].T, axis=0, keepdims=True), (8, steps))
    both = jnp.where(lax.broadcasted_iota(jnp.int32, (8, steps), 0) == 0, total, area)
    mine[...] = both
    swaps = []
    for k, p in enumerate(others):
        copy = pltpu.make_async_remote_copy(
            src_ref=mine,
            dst_ref=theirs.at[k],
            send_sem=ss.at[k],
            recv_sem=rs.at[k],
            device_id={"space": p},
            device_id_type=MESH,
        )
        copy.start()
        swaps.append(copy)
    for k, copy in enumerate(swaps):
        copy.wait()
        both = both + theirs[k]
    spread_ref[...] = both[0:1] / both[1:2]
    n = len(parts)
    landed(recv.at[:, pl.ds(0, slots)], sent.at[0])
    landed(recv.at[:, pl.ds(0, slots - 1)], sent.at[1])
    landed(recv.at[:, 0], sent.at[2])
    landed(stats.at[pl.ds(0, n * (slots - 1) * TABLE_ROWS)], sent.at[3])
    landed(stats.at[pl.ds(0, n * slots * TABLE_ROWS)], sent.at[4])


def on_device(thermal_reading, yearday_position, usable_observation_tally, location_surface_factor):
    groups, spaces = lax.axis_size("year"), lax.axis_size("space")
    steps, cells = thermal_reading.shape
    chunks = cells // LANES
    assert steps == LANES and chunks * LANES == cells
    pieces, _, parts = plan_of(groups, chunks)
    n_parts, slots = len(parts), len(parts[0][3])
    n_tiles = chunks // pieces
    n_others = max(spaces - 1, 1)

    tiles = thermal_reading.reshape(steps // 8, 8, chunks, LANES).transpose(0, 2, 1, 3)
    tiles = tiles.reshape(steps // 8, chunks * 8, LANES)
    vmem = pl.BlockSpec(memory_space=pltpu.VMEM)
    hbm = pl.BlockSpec(memory_space=pltpu.HBM)
    dma = pltpu.SemaphoreType.DMA

    def block(*shape):
        return pltpu.VMEM(shape, jnp.float32)

    departure, spread = pl.pallas_call(
        functools.partial(climate_kernel, groups, spaces, chunks),
        out_shape=(
            jax.ShapeDtypeStruct((steps * chunks, LANES), jnp.float32),
            jax.ShapeDtypeStruct((1, steps), jnp.float32),
        ),
        in_specs=[hbm, hbm, hbm, hbm],
        out_specs=(vmem, vmem),
        scratch_shapes=[block(steps // 8, pieces * 8, LANES) for _ in range(n_tiles)]
        + [block(pieces * TABLE_PITCH, LANES) for _ in range(n_tiles)]
        + [
            pltpu.VMEM((1, steps), jnp.int32),
            pltpu.VMEM((1, steps), jnp.int32),
            block(chunks, LANES),
            pltpu.VMEM((8, steps), jnp.int32),
            block(8, steps),
            pltpu.SMEM((8, steps), jnp.int32),
            pltpu.SMEM((8, steps), jnp.float32),
            block(3, steps + 1, pieces, LANES),
            block(chunks * STAT_PITCH, LANES),
            block(n_parts, slots + 1, STAT_ROWS, LANES),
            block(n_parts, 2 * slots, STAT_ROWS, LANES),
            block(steps, pieces, LANES),
            block(steps, LANES),
            block(8, steps),
            block(n_others, 8, steps),
            dma((n_tiles,)),
            dma((5,)),
            dma((5,)),
            dma((n_parts,)),
            dma((n_parts,)),
            dma((n_parts,)),
            dma((n_parts,)),
            dma((n_parts,)),
            dma((n_others,)),
            dma((n_others,)),
        ],
        compiler_params=pltpu.CompilerParams(
            collective_id=0, has_side_effects=True, vmem_limit_bytes=20 << 20
        ),
        name="climate",
    )(
        *[
            pltpu.with_memory_space_constraint(a, pltpu.HBM)
            for a in (
                tiles,
                yearday_position.reshape(1, steps),
                usable_observation_tally.reshape(1, steps),
                location_surface_factor.reshape(chunks, LANES),
            )
        ]
    )
    normalized_departure = (
        departure.reshape(steps // 8, chunks, 8, LANES).transpose(0, 2, 1, 3).reshape(steps, cells)
    )
    return normalized_departure, spread.reshape(steps)


def solution(mesh):
    return jax.shard_map(
        on_device,
        mesh=mesh,
        in_specs=(P("year", "space"), P("year"), P("year"), P("space")),
        out_specs=(P("year", "space"), P("year")),
        check_vma=False,
    )
```
